32 devices in a mesh: tm: 8 (over z, y), chan: 4 (over x, core).
Axes of the slice: x: 2, y: 2, z: 4, core: 2. Of those that a mesh axis runs over, the one named last changes fastest.
Arguments:
- coarse: bfloat16 [2, 24576, 4096], P(None, 'tm', 'chan'), may hold values from -6 to 6
- prototype: float32 [16, 1024], replicated, may hold values from -4 to 4
- req_block: int32 [4, 4], replicated, may hold values from 0 to 31, as said below
- req_start: int32 [4, 4], replicated, may hold values from 0 to 8, as said below
- req_frames: int32 [4, 4], replicated, may hold values from 1 to 9
- req_count: int32 [4], replicated, may hold values from 1 to 4, as said below
Outputs:
- spectra: bfloat16 [24, 4, 4, 2, 1024, 128], P('tm', 'chan')
The draws below stay inside these ranges and needn't reach their ends.
Inputs may be any that keep to these rules, and one draw needn't show every extreme that they name: `req_block`: among the live slots of one owner at most 2 name blocks b with the same b // 8; in every draw some owner reaches 2. req_start + req_frames <= 9 in every slot; in every draw some live slot starts at hop 9 - 1 and some live slot spans all 9 frames. Slots q < req_count[c] of owner c are live, the others are empty; in every draw some owner has 4 live slots.
All inputs are finite; a program needn't handle non-finite values.
Results may differ from the reference program's by a relative error of at most 0.001.
Values may be sent and summed in bfloat16 or wider, within the bound.
A program may use at most 256 MiB of HBM per device.

```python
import math
import jax
import jax.numpy as jnp
from jax import lax

CHANNELS = 4096
BLOCKW = 128
NFINE = 1024
TAPS = 16
MAXREQ = 4
PAIR = 2
OWNERS = 4
BPC = 8
TOTHOPS = 24
TIME = 24576
FRMAX = 9


def request_tables(key):
    count_key = jax.random.fold_in(key, 101)
    full_key = jax.random.fold_in(key, 102)
    base_key = jax.random.fold_in(key, 103)
    order_key = jax.random.fold_in(key, 104)
    inner_key = jax.random.fold_in(key, 105)
    frame_key = jax.random.fold_in(key, 106)
    start_key = jax.random.fold_in(key, 107)
    other_key = jax.random.fold_in(key, 108)
    lower_key = jax.random.fold_in(key, 109)
    owner_line = jnp.arange(OWNERS)
    slot_line = jnp.arange(MAXREQ)
    counts = jax.random.randint(count_key, (OWNERS,), 1, MAXREQ + 1)
    fullest = jax.random.randint(full_key, (), 0, OWNERS)
    smaller = (fullest + 1 + jax.random.randint(other_key, (), 0, OWNERS - 1)) % OWNERS
    lower_count = jax.random.randint(lower_key, (), 1, MAXREQ)
    counts = jnp.where(owner_line == smaller, lower_count, counts)
    counts = jnp.where(owner_line == fullest, MAXREQ, counts).astype(jnp.int32)
    bases = jax.random.randint(base_key, (OWNERS, 1), 0, OWNERS)
    order_keys = jax.random.split(order_key, OWNERS)
    orders = jax.vmap(lambda single: jax.random.permutation(single, MAXREQ))(order_keys)
    sources = (bases + orders // PAIR) % OWNERS
    blocks = (sources * BPC + jax.random.randint(inner_key, (OWNERS, MAXREQ), 0, BPC)).astype(jnp.int32)
    frames = jax.random.randint(frame_key, (OWNERS, MAXREQ), 1, FRMAX + 1)
    starts = jax.random.randint(start_key, (OWNERS, MAXREQ), 0, FRMAX + 1 - frames)
    is_full = owner_line[:, None] == fullest
    last_slot = is_full & (slot_line[None, :] == 0)
    whole_slot = is_full & (slot_line[None, :] == 1)
    frames = jnp.where(last_slot, 1, frames)
    frames = jnp.where(whole_slot, FRMAX, frames).astype(jnp.int32)
    starts = jnp.where(last_slot, FRMAX - 1, starts)
    starts = jnp.where(whole_slot, 0, starts).astype(jnp.int32)
    return (blocks, starts, frames, counts)


def draw_req_block(key, part):
    return request_tables(key)[0]


def draw_req_start(key, part):
    return request_tables(key)[1]


def draw_req_frames(key, part):
    return request_tables(key)[2]


def draw_req_count(key, part):
    return request_tables(key)[3]


def block_levels(own_key, extent, cuts, least, top_value):
    def one(dim, blocks):
        heights = jax.random.uniform(jax.random.fold_in(jax.random.fold_in(own_key, 6), dim), (blocks,), jnp.float32, least / len(cuts), top_value / len(cuts))
        return jnp.repeat(jnp.exp(heights), extent[dim] // blocks).reshape((-1,) + (1,) * (len(extent) - dim - 1))

    gain = one(*cuts[0])
    for cut in cuts[1:]:
        gain = gain * one(*cut)
    return gain


def scatter_about(key, extent, width, limit, cuts=(), kind=jnp.bfloat16):
    level = block_levels(key, extent, cuts, -0.22, 0.18) if cuts else 1.0
    values = jax.random.normal(key, extent, jnp.float32) * width * level
    return jnp.minimum(jnp.maximum(values, -limit), limit).astype(kind)


def setup_inputs(seed: int = 0) -> dict:
    seeds = jax.random.split(jax.random.key(seed), 7)
    return {
        "coarse": scatter_about(seeds[0], (2, TIME, CHANNELS), 1.0, 6.0, ((1, 8), (2, 4))),
        "prototype": scatter_about(seeds[1], (TAPS, NFINE), (TAPS ** -0.5), 4.0, (), jnp.float32),
        "req_block": draw_req_block(jax.random.fold_in(seeds[6], 71), 0),
        "req_start": draw_req_start(jax.random.fold_in(seeds[6], 71), 0),
        "req_frames": draw_req_frames(jax.random.fold_in(seeds[6], 71), 0),
        "req_count": draw_req_count(jax.random.fold_in(seeds[6], 71), 0),
    }


def reference(coarse, prototype, req_block, req_start, req_frames, req_count):
    hop_ids = jnp.arange(TOTHOPS, dtype=jnp.int32)
    results = []
    for owner in range(OWNERS):
        for slot_index in range(MAXREQ):
            first_col = (req_block[owner, slot_index] * BLOCKW).astype(jnp.int32)
            block_data = lax.dynamic_slice(coarse, (jnp.int32(0), jnp.int32(0), first_col), (2, TIME, BLOCKW))
            block_data = block_data.astype(jnp.float32).reshape(2, TOTHOPS, NFINE, BLOCKW)
            padding = jnp.zeros((2, TAPS - 1, NFINE, BLOCKW), jnp.float32)
            padded = jnp.concatenate([block_data, padding.astype(block_data.dtype)], axis=1)
            filtered = jnp.zeros((2, TOTHOPS, NFINE, BLOCKW), block_data.dtype)
            for tap_index in range(TAPS):
                weights = prototype[tap_index][None, None, :, None]
                filtered = filtered + weights * padded[:, tap_index:tap_index + TOTHOPS]
            transformed = jnp.fft.fft(filtered[0] + 1j * filtered[1], axis=1) / math.sqrt(NFINE)
            stacked = jnp.stack([jnp.real(transformed), jnp.imag(transformed)], axis=1)
            begin = req_start[owner, slot_index]
            active = (slot_index < req_count[owner]) & (hop_ids >= begin) & (hop_ids < begin + req_frames[owner, slot_index])
            masked = jnp.where(active[:, None, None, None], stacked, jnp.zeros_like(stacked))
            results.append(masked.astype(jnp.bfloat16))
    spectra = jnp.stack(results, axis=1)
    return spectra.reshape(TOTHOPS, OWNERS, MAXREQ, 2, NFINE, BLOCKW)
```

```python
import functools
import math

import jax
import jax.numpy as jnp
import numpy as np
from jax import lax
from jax.experimental import pallas as pl
from jax.experimental.pallas import tpu as pltpu
from jax.sharding import PartitionSpec as P

BLOCKW = 128
NFINE = 1024
TAPS = 16
MAXREQ = 4
PAIR = 2
CHUNKS = 3
ANY = pl.BlockSpec(memory_space=pl.ANY)


def build_table():
    line = jnp.arange(NFINE, dtype=jnp.int32)
    products = line[:, None] * line[None, :] % NFINE
    angles = products.astype(jnp.float32) * (2.0 * math.pi / NFINE)
    scale = 1.0 / math.sqrt(NFINE)
    return jnp.concatenate([jnp.cos(angles) * scale, jnp.sin(angles) * scale], axis=0)


def pack_kernel(chosen, coarse_ref, out_ref):
    out_ref[...] = coarse_ref[...].reshape(out_ref.shape)


def pack(coarse, chosen, first, hops):
    count = chosen.shape[0]
    return pl.pallas_call(
        pack_kernel,
        out_shape=jax.ShapeDtypeStruct((count, 2, hops * NFINE, BLOCKW), coarse.dtype),
        grid_spec=pltpu.PrefetchScalarGridSpec(
            num_scalar_prefetch=1,
            grid=(count,),
            in_specs=[pl.BlockSpec((2, hops * NFINE, BLOCKW), lambda i, c: (0, first, c[i]))],
            out_specs=pl.BlockSpec((1, 2, hops * NFINE, BLOCKW), lambda i, c: (i, 0, 0, 0)),
        ),
        cost_estimate=pl.CostEstimate(
            flops=0, transcendentals=0, bytes_accessed=count * 8 * hops * NFINE * BLOCKW
        ),
    )(chosen, coarse)


def select_kernel(pieces, arrival, in_ref, out_ref):
    share = BLOCKW // pieces
    for piece in range(pieces):
        cols = slice(piece * share, (piece + 1) * share)
        out_ref[piece] = jnp.concatenate([in_ref[0, 0, :, cols], in_ref[0, 1, :, cols]], axis=-1)


def select(incoming, arrival, pieces, hops):
    width = 2 * BLOCKW // pieces
    rows = hops * NFINE
    return pl.pallas_call(
        functools.partial(select_kernel, pieces),
        out_shape=jax.ShapeDtypeStruct((MAXREQ * pieces, rows, width), incoming.dtype),
        grid_spec=pltpu.PrefetchScalarGridSpec(
            num_scalar_prefetch=1,
            grid=(MAXREQ, hops),
            in_specs=[pl.BlockSpec((1, 2, NFINE, BLOCKW), lambda q, h, a: (a[q], 0, h, 0))],
            out_specs=pl.BlockSpec((pieces, NFINE, width), lambda q, h, a: (q, h, 0)),
        ),
        cost_estimate=pl.CostEstimate(
            flops=0, transcendentals=0, bytes_accessed=MAXREQ * 8 * rows * BLOCKW
        ),
    )(arrival, incoming)


def return_kernel(size, keepers, hops, res_ref, out_ref, send_sems, recv_sems):
    me = lax.axis_index("tm")
    barrier = pltpu.get_barrier_semaphore()

    @pl.loop(1, size)
    def _(step):
        other = lax.rem(me + step, size)
        pl.semaphore_signal(barrier, inc=1, device_id={"tm": other})

    pl.semaphore_wait(barrier, size - 1)

    def copy(step):
        target = lax.rem(me + step, size)
        return pltpu.make_async_remote_copy(
            src_ref=res_ref.at[pl.ds(target * hops, hops)],
            dst_ref=out_ref.at[me],
            send_sem=send_sems.at[step],
            recv_sem=recv_sems.at[step],
            device_id={"tm": target},
        )

    def arriving(step):
        source = lax.rem(me + size - step, size)
        return pltpu.make_async_remote_copy(
            src_ref=res_ref.at[pl.ds(0, hops)],
            dst_ref=out_ref.at[source],
            send_sem=send_sems.at[step],
            recv_sem=recv_sems.at[step],
            device_id={"tm": source},
        )

    @pl.loop(1, size)
    def _(step):
        @pl.when(lax.rem(me + step, size) < keepers)
        def _():
            copy(step).start()

    @pl.when(me < keepers)
    def _():
        @pl.loop(1, size)
        def _(step):
            arriving(step).wait_recv()

    @pl.loop(1, size)
    def _(step):
        @pl.when(lax.rem(me + step, size) < keepers)
        def _():
            copy(step).wait_send()


def give_back(result, size, keepers, hops):
    shape = (size, hops) + result.shape[1:]
    return pl.pallas_call(
        functools.partial(return_kernel, size, keepers, hops),
        out_shape=jax.ShapeDtypeStruct(shape, result.dtype),
        in_specs=[ANY],
        out_specs=ANY,
        scratch_shapes=[pltpu.SemaphoreType.DMA((size,)), pltpu.SemaphoreType.DMA((size,))],
        compiler_params=pltpu.CompilerParams(collective_id=0, has_side_effects=True),
    )(result)


def final_kernel(pieces, meta, got_ref, own_ref, out_ref):
    share = BLOCKW // pieces
    slot, hop = pl.program_id(0), pl.program_id(1)
    row = meta[0]
    active = meta[2 + slot * pl.num_programs(1) + hop] > 0

    @pl.when(jnp.logical_not(active))
    def _():
        out_ref[...] = jnp.zeros_like(out_ref)

    @pl.when(active)
    def _():
        data = [
            jnp.where(slot * pieces + piece == row, own_ref[0], got_ref[piece, 0])
            for piece in range(pieces)
        ]
        for part in range(2):
            cols = slice(part * share, (part + 1) * share)
            out_ref[0, 0, part] = jnp.concatenate([d[:, cols] for d in data], axis=-1)


def assemble(got, result, active, row, keepers, pieces):
    size, hops, _, width = got.shape
    base = jnp.minimum(row, keepers - 1) * hops
    meta = jnp.concatenate(
        [jnp.stack([row, base]).astype(jnp.int32), active.astype(jnp.int32).reshape(-1)]
    )
    return pl.pallas_call(
        functools.partial(final_kernel, pieces),
        out_shape=jax.ShapeDtypeStruct((hops, MAXREQ, 2, NFINE, BLOCKW), got.dtype),
        grid_spec=pltpu.PrefetchScalarGridSpec(
            num_scalar_prefetch=1,
            grid=(MAXREQ, hops),
            in_specs=[
                pl.BlockSpec((pieces, 1, NFINE, width), lambda q, h, m: (q, h, 0, 0)),
                pl.BlockSpec((1, NFINE, width), lambda q, h, m: (m[1] + h, 0, 0)),
            ],
            out_specs=pl.BlockSpec((1, 1, 2, NFINE, BLOCKW), lambda q, h, m: (h, q, 0, 0, 0)),
        ),
    )(meta, got, result)


def shards(coarse, prototype, req_block, req_start, req_frames, req_count):
    owners = lax.axis_size("chan")
    column = lax.axis_index("chan")
    row = lax.axis_index("tm")
    size = lax.axis_size("tm")
    per_column = coarse.shape[2] // BLOCKW
    hops = coarse.shape[1] // NFINE
    all_hops = hops * size
    frames = all_hops - TAPS + 1
    keepers = -(-frames // hops)
    pieces = size // MAXREQ
    width = 2 * BLOCKW // pieces
    share = BLOCKW // pieces

    slot_ids = jnp.arange(MAXREQ, dtype=jnp.int32)
    live = slot_ids[None, :] < req_count[:, None]
    sources = req_block // per_column
    same = (
        live[:, :, None]
        & live[:, None, :]
        & (sources[:, :, None] == sources[:, None, :])
        & (slot_ids[None, None, :] < slot_ids[None, :, None])
    )
    rank = jnp.sum(same.astype(jnp.int32), axis=2)
    picked = (
        (live & (sources == column))[:, None, :]
        & (rank[:, None, :] == jnp.arange(PAIR, dtype=jnp.int32)[None, :, None])
    )
    local = req_block - column * per_column
    chosen = jnp.sum(jnp.where(picked, local[:, None, :], 0), axis=2).reshape(-1)
    chosen = jnp.clip(chosen, 0, per_column - 1).astype(jnp.int32)
    mine = (jnp.arange(owners, dtype=jnp.int32) == column)[:, None]

    def own(table):
        return jnp.sum(jnp.where(mine, table, 0), axis=0)

    my_live = slot_ids < own(req_count[:, None])[0]
    arrival = jnp.where(my_live, own(sources) * PAIR + own(rank), 0)
    arrival = jnp.clip(arrival, 0, owners * PAIR - 1).astype(jnp.int32)
    my_start, my_frames = own(req_start), own(req_frames)
    hop_ids = row * hops + jnp.arange(hops, dtype=jnp.int32)
    active = (
        my_live[:, None]
        & (hop_ids[None, :] >= my_start[:, None])
        & (hop_ids[None, :] < (my_start + my_frames)[:, None])
    )

    table = build_table()
    chunks = CHUNKS if hops % CHUNKS == 0 else 1
    per_chunk = hops // chunks
    parts = []
    for chunk in range(chunks):
        outgoing = pack(coarse, chosen, chunk, per_chunk)
        incoming = lax.all_to_all(outgoing, "chan", split_axis=0, concat_axis=0, tiled=True)
        sending = select(incoming, arrival, pieces, per_chunk)
        gathered = lax.all_to_all(sending, "tm", split_axis=0, concat_axis=0, tiled=True)
        parts.append(gathered.reshape(size, per_chunk, NFINE, width))
    samples = [
        parts[(h % hops) // per_chunk][h // hops, (h % hops) % per_chunk] for h in range(all_hops)
    ]
    filtered = []
    for frame in range(frames):
        total = None
        for tap in range(TAPS):
            term = prototype[tap][:, None] * samples[frame + tap].astype(jnp.float32)
            total = term if total is None else total + term
        filtered.append(total)
    flat = jnp.concatenate(filtered, axis=1)
    both = jnp.dot(table, flat, precision=lax.Precision.HIGH, preferred_element_type=jnp.float32)
    both = both.reshape(2, NFINE, frames, 2, share)
    cosine, sine = both[0], both[1]
    result = jnp.stack(
        [cosine[:, :, 0] + sine[:, :, 1], cosine[:, :, 1] - sine[:, :, 0]], axis=2
    ).astype(jnp.bfloat16)
    result = result.reshape(NFINE, frames, width).transpose(1, 0, 2)
    extra = keepers * hops - frames
    if extra:
        result = jnp.concatenate([result, jnp.zeros((extra, NFINE, width), result.dtype)], axis=0)
    got = give_back(result, size, keepers, hops)
    return assemble(got, result, active, row, keepers, pieces)[:, None]


def solution(mesh):
    return jax.shard_map(
        shards,
        mesh=mesh,
        in_specs=(P(None, "tm", "chan"), P(), P(), P(), P(), P()),
        out_specs=P("tm", "chan", None, None, None, None),
        check_vma=False,
    )
```

```python
import functools
import math

import jax
import jax.numpy as jnp
from jax import lax
from jax.experimental import pallas as pl
from jax.experimental.pallas import tpu as pltpu
from jax.sharding import PartitionSpec as P

BLOCKW = 128
NFINE = 1024
TAPS = 16
MAXREQ = 4
PAIR = 2
ROWS = 128
STEP = 16
ANY = pl.BlockSpec(memory_space=pl.ANY)


def build_table():
    line = jnp.arange(NFINE, dtype=jnp.int32)
    products = line[:, None] * line[None, :] % NFINE
    angles = products.astype(jnp.float32) * (2.0 * math.pi / NFINE)
    scale = 1.0 / math.sqrt(NFINE)
    return jnp.concatenate([jnp.cos(angles) * scale, jnp.sin(angles) * scale], axis=0)


def pack_kernel(chosen, coarse_ref, out_ref):
    out_ref[...] = coarse_ref[...].reshape(out_ref.shape)


def pack(coarse, chosen, first, hops):
    count = chosen.shape[0]
    return pl.pallas_call(
        pack_kernel,
        out_shape=jax.ShapeDtypeStruct((count, 2, hops * NFINE, BLOCKW), coarse.dtype),
        grid_spec=pltpu.PrefetchScalarGridSpec(
            num_scalar_prefetch=1,
            grid=(count,),
            in_specs=[pl.BlockSpec((2, hops * NFINE, BLOCKW), lambda i, c: (0, first, c[i]))],
            out_specs=pl.BlockSpec((1, 2, hops * NFINE, BLOCKW), lambda i, c: (i, 0, 0, 0)),
        ),
        cost_estimate=pl.CostEstimate(
            flops=0, transcendentals=0, bytes_accessed=count * 8 * hops * NFINE * BLOCKW
        ),
    )(chosen, coarse)


def select_kernel(pieces, arrival, in_ref, out_ref):
    share = BLOCKW // pieces
    for piece in range(pieces):
        cols = slice(piece * share, (piece + 1) * share)
        out_ref[piece] = jnp.concatenate([in_ref[0, 0, :, cols], in_ref[0, 1, :, cols]], axis=-1)


def select(incoming, arrival, pieces, hops):
    width = 2 * BLOCKW // pieces
    rows = hops * NFINE
    return pl.pallas_call(
        functools.partial(select_kernel, pieces),
        out_shape=jax.ShapeDtypeStruct((MAXREQ * pieces, rows, width), incoming.dtype),
        grid_spec=pltpu.PrefetchScalarGridSpec(
            num_scalar_prefetch=1,
            grid=(MAXREQ, hops),
            in_specs=[pl.BlockSpec((1, 2, NFINE, BLOCKW), lambda q, h, a: (a[q], 0, h, 0))],
            out_specs=pl.BlockSpec((pieces, NFINE, width), lambda q, h, a: (q, h, 0)),
        ),
        cost_estimate=pl.CostEstimate(
            flops=0, transcendentals=0, bytes_accessed=MAXREQ * 8 * rows * BLOCKW
        ),
    )(arrival, incoming)


def exchange_kernel(
    owners, size, a_in, b_in, a_out, b_out, a_tmp, b_tmp, a_send, a_recv, b_send, b_recv, local
):
    column, row = lax.axis_index("chan"), lax.axis_index("tm")
    barrier = pltpu.get_barrier_semaphore()

    @pl.loop(1, owners)
    def _(step):
        other = lax.rem(column + step, owners)
        pl.semaphore_signal(barrier, inc=1, device_id={"chan": other})

    @pl.loop(1, size)
    def _(step):
        other = lax.rem(row + step, size)
        pl.semaphore_signal(barrier, inc=1, device_id={"tm": other})

    pl.semaphore_wait(barrier, owners + size - 2)

    def a_copy(step, source, target, device):
        return pltpu.make_async_remote_copy(
            src_ref=a_in.at[pl.ds(target * PAIR, PAIR)],
            dst_ref=a_out.at[pl.ds(source * PAIR, PAIR)],
            send_sem=a_send.at[step],
            recv_sem=a_recv.at[step],
            device_id={"chan": device},
        )

    def b_copy(step, source, target, device):
        return pltpu.make_async_remote_copy(
            src_ref=b_in.at[target],
            dst_ref=b_out.at[source],
            send_sem=b_send.at[step],
            recv_sem=b_recv.at[step],
            device_id={"tm": device},
        )

    @pl.loop(1, size)
    def _(step):
        target = lax.rem(row + step, size)
        b_copy(step, row, target, target).start()

    @pl.loop(1, owners)
    def _(step):
        target = lax.rem(column + step, owners)
        a_copy(step, column, target, target).start()

    a_read = pltpu.make_async_copy(a_in.at[pl.ds(column * PAIR, PAIR)], a_tmp, local.at[0])
    b_read = pltpu.make_async_copy(b_in.at[row], b_tmp, local.at[1])
    a_read.start()
    b_read.start()
    a_read.wait()
    b_read.wait()
    a_write = pltpu.make_async_copy(a_tmp, a_out.at[pl.ds(column * PAIR, PAIR)], local.at[2])
    b_write = pltpu.make_async_copy(b_tmp, b_out.at[row], local.at[3])
    a_write.start()
    b_write.start()
    a_write.wait()
    b_write.wait()

    @pl.loop(1, owners)
    def _(step):
        source = lax.rem(column + owners - step, owners)
        copy = a_copy(step, source, column, source)
        copy.wait_recv()
        copy.wait_send()

    @pl.loop(1, size)
    def _(step):
        source = lax.rem(row + size - step, size)
        copy = b_copy(step, source, row, source)
        copy.wait_recv()
        copy.wait_send()


def exchange(outgoing, sending, owners, size, collective):
    sem = pltpu.SemaphoreType.DMA
    return pl.pallas_call(
        functools.partial(exchange_kernel, owners, size),
        out_shape=(
            jax.ShapeDtypeStruct(outgoing.shape, outgoing.dtype),
            jax.ShapeDtypeStruct(sending.shape, sending.dtype),
        ),
        in_specs=[ANY, ANY],
        out_specs=(ANY, ANY),
        scratch_shapes=[
            pltpu.VMEM((PAIR,) + outgoing.shape[1:], outgoing.dtype),
            pltpu.VMEM(sending.shape[1:], sending.dtype),
            sem((owners,)),
            sem((owners,)),
            sem((size,)),
            sem((size,)),
            sem((4,)),
        ],
        compiler_params=pltpu.CompilerParams(collective_id=collective, has_side_effects=True),
    )(outgoing, sending)


def filter_kernel(hops, frames, weights_ref, *refs):
    out_ref = refs[-1]
    width = refs[0].shape[-1]

    @pl.loop(0, ROWS // STEP)
    def _(step):
        rows = pl.ds(pl.multiple_of(step * STEP, STEP), STEP)
        weights = [
            jnp.broadcast_to(weights_ref[rows, tap : tap + 1], (STEP, width)) for tap in range(TAPS)
        ]
        for frame in range(frames):
            total = None
            for tap in range(TAPS):
                hop = frame + tap
                term = weights[tap] * refs[hop % hops][hop // hops, rows, :].astype(jnp.float32)
                total = term if total is None else total + term
            out_ref[rows, frame * width : (frame + 1) * width] = total


def polyphase(parts, prototype, frames):
    hops = len(parts)
    size, _, width = parts[0].shape
    return pl.pallas_call(
        functools.partial(filter_kernel, hops, frames),
        out_shape=jax.ShapeDtypeStruct((NFINE, frames * width), jnp.float32),
        grid=(NFINE // ROWS,),
        in_specs=[pl.BlockSpec((ROWS, TAPS), lambda i: (i, 0))]
        + [pl.BlockSpec((size, ROWS, width), lambda i: (0, i, 0))] * hops,
        out_specs=pl.BlockSpec((ROWS, frames * width), lambda i: (i, 0)),
    )(prototype.T, *parts)


def combine_kernel(frames, share, both_ref, out_ref):
    frame = pl.program_id(0)

    @pl.when(frame < frames)
    def _():
        sine = both_ref[1]
        turned = jnp.concatenate([sine[:, share:], -sine[:, :share]], axis=-1)
        out_ref[0] = (both_ref[0] + turned).astype(out_ref.dtype)

    @pl.when(frame >= frames)
    def _():
        out_ref[...] = jnp.zeros_like(out_ref)


def combine(both, frames, padded, width):
    return pl.pallas_call(
        functools.partial(combine_kernel, frames, width // 2),
        out_shape=jax.ShapeDtypeStruct((padded, NFINE, width), jnp.bfloat16),
        grid=(padded,),
        in_specs=[
            pl.BlockSpec((2, NFINE, width), lambda f: (0, 0, jnp.minimum(f, frames - 1))),
        ],
        out_specs=pl.BlockSpec((1, NFINE, width), lambda f: (f, 0, 0)),
    )(both)


def return_kernel(size, keepers, hops, res_ref, out_ref, send_sems, recv_sems):
    me = lax.axis_index("tm")
    barrier = pltpu.get_barrier_semaphore()

    @pl.loop(1, size)
    def _(step):
        other = lax.rem(me + step, size)
        pl.semaphore_signal(barrier, inc=1, device_id={"tm": other})

    pl.semaphore_wait(barrier, size - 1)

    def copy(step):
        target = lax.rem(me + step, size)
        return pltpu.make_async_remote_copy(
            src_ref=res_ref.at[pl.ds(target * hops, hops)],
            dst_ref=out_ref.at[me],
            send_sem=send_sems.at[step],
            recv_sem=recv_sems.at[step],
            device_id={"tm": target},
        )

    def arriving(step):
        source = lax.rem(me + size - step, size)
        return pltpu.make_async_remote_copy(
            src_ref=res_ref.at[pl.ds(0, hops)],
            dst_ref=out_ref.at[source],
            send_sem=send_sems.at[step],
            recv_sem=recv_sems.at[step],
            device_id={"tm": source},
        )

    @pl.loop(1, size)
    def _(step):
        @pl.when(lax.rem(me + step, size) < keepers)
        def _():
            copy(step).start()

    @pl.when(me < keepers)
    def _():
        @pl.loop(1, size)
        def _(step):
            arriving(step).wait_recv()

    @pl.loop(1, size)
    def _(step):
        @pl.when(lax.rem(me + step, size) < keepers)
        def _():
            copy(step).wait_send()


def give_back(result, size, keepers, hops):
    shape = (size, hops) + result.shape[1:]
    return pl.pallas_call(
        functools.partial(return_kernel, size, keepers, hops),
        out_shape=jax.ShapeDtypeStruct(shape, result.dtype),
        in_specs=[ANY],
        out_specs=ANY,
        scratch_shapes=[pltpu.SemaphoreType.DMA((size,)), pltpu.SemaphoreType.DMA((size,))],
        compiler_params=pltpu.CompilerParams(collective_id=0, has_side_effects=True),
    )(result)


def final_kernel(pieces, meta, got_ref, own_ref, out_ref):
    share = BLOCKW // pieces
    slot, hop = pl.program_id(0), pl.program_id(1)
    row = meta[0]
    active = meta[2 + slot * pl.num_programs(1) + hop] > 0

    @pl.when(jnp.logical_not(active))
    def _():
        out_ref[...] = jnp.zeros_like(out_ref)

    @pl.when(active)
    def _():
        data = [
            jnp.where(slot * pieces + piece == row, own_ref[0], got_ref[piece, 0])
            for piece in range(pieces)
        ]
        for part in range(2):
            cols = slice(part * share, (part + 1) * share)
            out_ref[0, 0, part] = jnp.concatenate([d[:, cols] for d in data], axis=-1)


def assemble(got, result, active, row, keepers, pieces):
    size, hops, _, width = got.shape
    base = jnp.minimum(row, keepers - 1) * hops
    meta = jnp.concatenate(
        [jnp.stack([row, base]).astype(jnp.int32), active.astype(jnp.int32).reshape(-1)]
    )
    return pl.pallas_call(
        functools.partial(final_kernel, pieces),
        out_shape=jax.ShapeDtypeStruct((hops, MAXREQ, 2, NFINE, BLOCKW), got.dtype),
        grid_spec=pltpu.PrefetchScalarGridSpec(
            num_scalar_prefetch=1,
            grid=(MAXREQ, hops),
            in_specs=[
                pl.BlockSpec((pieces, 1, NFINE, width), lambda q, h, m: (q, h, 0, 0)),
                pl.BlockSpec((1, NFINE, width), lambda q, h, m: (m[1] + h, 0, 0)),
            ],
            out_specs=pl.BlockSpec((1, 1, 2, NFINE, BLOCKW), lambda q, h, m: (h, q, 0, 0, 0)),
        ),
    )(meta, got, result)


def shards(coarse, prototype, req_block, req_start, req_frames, req_count):
    owners = lax.axis_size("chan")
    column = lax.axis_index("chan")
    row = lax.axis_index("tm")
    size = lax.axis_size("tm")
    per_column = coarse.shape[2] // BLOCKW
    hops = coarse.shape[1] // NFINE
    all_hops = hops * size
    frames = all_hops - TAPS + 1
    keepers = -(-frames // hops)
    pieces = size // MAXREQ
    width = 2 * BLOCKW // pieces
    share = BLOCKW // pieces

    slot_ids = jnp.arange(MAXREQ, dtype=jnp.int32)
    live = slot_ids[None, :] < req_count[:, None]
    sources = req_block // per_column
    same = (
        live[:, :, None]
        & live[:, None, :]
        & (sources[:, :, None] == sources[:, None, :])
        & (slot_ids[None, None, :] < slot_ids[None, :, None])
    )
    rank = jnp.sum(same.astype(jnp.int32), axis=2)
    picked = (
        (live & (sources == column))[:, None, :]
        & (rank[:, None, :] == jnp.arange(PAIR, dtype=jnp.int32)[None, :, None])
    )
    local = req_block - column * per_column
    chosen = jnp.sum(jnp.where(picked, local[:, None, :], 0), axis=2).reshape(-1)
    chosen = jnp.clip(chosen, 0, per_column - 1).astype(jnp.int32)
    mine = (jnp.arange(owners, dtype=jnp.int32) == column)[:, None]

    def own(table):
        return jnp.sum(jnp.where(mine, table, 0), axis=0)

    my_live = slot_ids < own(req_count[:, None])[0]
    arrival = jnp.where(my_live, own(sources) * PAIR + own(rank), 0)
    arrival = jnp.clip(arrival, 0, owners * PAIR - 1).astype(jnp.int32)
    my_start, my_frames = own(req_start), own(req_frames)
    hop_ids = row * hops + jnp.arange(hops, dtype=jnp.int32)
    active = (
        my_live[:, None]
        & (hop_ids[None, :] >= my_start[:, None])
        & (hop_ids[None, :] < (my_start + my_frames)[:, None])
    )

    table = build_table()
    outgoing = [pack(coarse, chosen, hop, 1) for hop in range(hops)]
    incoming = lax.all_to_all(outgoing[0], "chan", split_axis=0, concat_axis=0, tiled=True)
    parts = []
    for hop in range(1, hops):
        sending = select(incoming, arrival, pieces, 1)
        incoming, gathered = exchange(outgoing[hop], sending, owners, size, hop)
        parts.append(gathered)
    sending = select(incoming, arrival, pieces, 1)
    parts.append(lax.all_to_all(sending, "tm", split_axis=0, concat_axis=0, tiled=True))
    flat = polyphase(parts, prototype, frames)
    both = jnp.dot(table, flat, precision=lax.Precision.HIGH, preferred_element_type=jnp.float32)
    padded = keepers * hops
    if width % 128 == 0:
        result = combine(both.reshape(2, NFINE, frames * width), frames, padded, width)
    else:
        both = both.reshape(2, NFINE, frames, 2, share)
        cosine, sine = both[0], both[1]
        result = jnp.stack(
            [cosine[:, :, 0] + sine[:, :, 1], cosine[:, :, 1] - sine[:, :, 0]], axis=2
        ).astype(jnp.bfloat16)
        result = result.reshape(NFINE, frames, width).transpose(1, 0, 2)
        if padded > frames:
            zeros = jnp.zeros((padded - frames, NFINE, width), result.dtype)
            result = jnp.concatenate([result, zeros], axis=0)
    got = give_back(result, size, keepers, hops)
    return assemble(got, result, active, row, keepers, pieces)[:, None]


def solution(mesh):
    return jax.shard_map(
        shards,
        mesh=mesh,
        in_specs=(P(None, "tm", "chan"), P(), P(), P(), P(), P()),
        out_specs=P("tm", "chan", None, None, None, None),
        check_vma=False,
    )
```
